8 devices in a mesh: data: 2 (over z, y), stage: 4 (over x, core).
Axes of the slice: x: 2, y: 2, z: 1, core: 2. Of those that a mesh axis runs over, the one named last changes fastest.
Arguments:
- acts_in: bfloat16 [16, 4096, 768], P(('data', 'stage')), parts along dimension 0
- grad_out: bfloat16 [16, 4096, 768], P(('data', 'stage')), parts along dimension 0
- w_up_a: bfloat16 [4, 768, 3072], P('stage')
- w_down_a: bfloat16 [4, 3072, 768], P('stage')
- w_up_b: bfloat16 [4, 768, 768], P('stage')
- w_down_b: bfloat16 [4, 768, 768], P('stage')
Outputs:
- output 1: bfloat16 [16, 4096, 768], P(('data', 'stage')), parts along dimension 0
- output 2: bfloat16 [16, 4096, 768], P(('data', 'stage')), parts along dimension 0
- output 3: float32 [8, 768, 3072], P(('data', 'stage')), parts along dimension 0
- output 4: float32 [8, 3072, 768], P(('data', 'stage')), parts along dimension 0
- output 5: float32 [8, 768, 768], P(('data', 'stage')), parts along dimension 0
- output 6: float32 [8, 768, 768], P(('data', 'stage')), parts along dimension 0
There are 2 independent parts. The reference program is written for one: setup_inputs(seed, part) draws one part's arguments, and reference() takes and returns one part's arrays. A program takes and returns all parts, laid end to end along the dimension named above; an argument that names none is the same for every part.
All inputs are finite; a program needn't handle non-finite values.
Results may differ from the reference program's by a relative error of at most 0.0163569.
Values are sent between devices in bfloat16 or wider.
A program may use at most 1 GiB of HBM per device.

```python
import jax
import jax.numpy as jnp
from jax import lax

D_MODEL = 768
D_FF = 3072
STAGES = 4
ROUNDS = 1
N_MICRO = 8
TOKENS = 4096

PAIRS = ROUNDS * STAGES
NARROW = D_FF // 4
LAYERS = 2 * PAIRS


def setup_inputs(seed: int = 0, part: int = 0) -> dict:
    data_root, weight_root = jax.random.split(jax.random.key(seed), 2)
    part_key = jax.random.fold_in(data_root, part)
    key_acts, key_grad = jax.random.split(part_key, 2)
    key_up_a, key_down_a, key_up_b, key_down_b = jax.random.split(weight_root, 4)
    depth_gain = (3.0 / LAYERS) ** 0.5
    acts_in = jax.random.normal(key_acts, (N_MICRO, TOKENS, D_MODEL), jnp.float32)
    grad_out = jax.random.normal(key_grad, (N_MICRO, TOKENS, D_MODEL), jnp.float32)
    w_up_a = jax.random.normal(key_up_a, (PAIRS, D_MODEL, D_FF), jnp.float32) * (D_MODEL ** -0.5)
    w_down_a = jax.random.normal(key_down_a, (PAIRS, D_FF, D_MODEL), jnp.float32) * (depth_gain * D_FF ** -0.5)
    w_up_b = jax.random.normal(key_up_b, (PAIRS, D_MODEL, NARROW), jnp.float32) * (D_MODEL ** -0.5)
    w_down_b = jax.random.normal(key_down_b, (PAIRS, NARROW, D_MODEL), jnp.float32) * (depth_gain * NARROW ** -0.5)
    return dict(acts_in=acts_in.astype(jnp.bfloat16), grad_out=grad_out.astype(jnp.bfloat16), w_up_a=w_up_a.astype(jnp.bfloat16), w_down_a=w_down_a.astype(jnp.bfloat16), w_up_b=w_up_b.astype(jnp.bfloat16), w_down_b=w_down_b.astype(jnp.bfloat16))


def layer_forward(hidden, w_up, w_down):
    pre_act = jnp.dot(hidden, w_up, preferred_element_type=jnp.float32)
    gelu_out = jax.nn.gelu(pre_act).astype(jnp.bfloat16)
    resid_delta = jnp.dot(gelu_out, w_down, preferred_element_type=jnp.float32)
    return (hidden.astype(jnp.float32) + resid_delta).astype(jnp.bfloat16)


def layer_backward(hidden, w_up, w_down, grad_next):
    pre_act = jnp.dot(hidden, w_up, preferred_element_type=jnp.float32)
    gelu_val, gelu_pull = jax.vjp(jax.nn.gelu, pre_act)
    gelu_out = gelu_val.astype(jnp.bfloat16)
    dw_down = jnp.dot(gelu_out.T, grad_next, preferred_element_type=jnp.float32)
    d_gelu = jnp.dot(grad_next, w_down.T, preferred_element_type=jnp.float32)
    d_pre = gelu_pull(d_gelu)[0].astype(jnp.bfloat16)
    dw_up = jnp.dot(hidden.T, d_pre, preferred_element_type=jnp.float32)
    back_prod = jnp.dot(d_pre, w_up.T, preferred_element_type=jnp.float32)
    grad_prev = (grad_next.astype(jnp.float32) + back_prod).astype(jnp.bfloat16)
    return grad_prev, dw_up, dw_down


def to_pair_order(weight):
    return weight.reshape((STAGES, ROUNDS) + weight.shape[1:]).swapaxes(0, 1).reshape(weight.shape)


def from_pair_order(grad_stack):
    return grad_stack.reshape((ROUNDS, STAGES) + grad_stack.shape[1:]).swapaxes(0, 1).reshape(grad_stack.shape)


def pair_forward(hidden, pair_weights):
    up_a, down_a, up_b, down_b = pair_weights
    mid_hidden = layer_forward(hidden, up_a, down_a)
    return layer_forward(mid_hidden, up_b, down_b), (hidden, mid_hidden)


def pair_backward(grad_next, step_in):
    (hidden, mid_hidden), (up_a, down_a, up_b, down_b) = step_in
    grad_mid, dw_up_b, dw_down_b = layer_backward(mid_hidden, up_b, down_b, grad_next)
    grad_prev, dw_up_a, dw_down_a = layer_backward(hidden, up_a, down_a, grad_mid)
    return grad_prev, (dw_up_a, dw_down_a, dw_up_b, dw_down_b)


def reference(acts_in, grad_out, w_up_a, w_down_a, w_up_b, w_down_b):
    ordered = tuple(to_pair_order(weight) for weight in (w_up_a, w_down_a, w_up_b, w_down_b))

    def micro_step(grad_sums, micro_in):
        micro_acts, micro_grad = micro_in
        last_hidden, saved_acts = lax.scan(pair_forward, micro_acts, ordered)
        first_grad, pair_grads = lax.scan(pair_backward, micro_grad, (saved_acts, ordered), reverse=True)
        new_sums = tuple(run_sum + micro_part for run_sum, micro_part in zip(grad_sums, pair_grads))
        return new_sums, (last_hidden, first_grad)

    zero_sums = tuple(jnp.zeros(weight.shape, jnp.float32) for weight in ordered)
    grad_sums, (acts_out, grad_in) = lax.scan(micro_step, zero_sums, (acts_in, grad_out))
    weight_grads = tuple(from_pair_order(grad_stack) for grad_stack in grad_sums)
    return (acts_out, grad_in, weight_grads[0], weight_grads[1], weight_grads[2], weight_grads[3])
```

```python
import functools

import jax
import jax.numpy as jnp
from jax import lax
from jax.experimental import pallas as pl
from jax.experimental.pallas import tpu as pltpu
from jax.sharding import PartitionSpec as P

BF = jnp.bfloat16
F32 = jnp.float32
SDS = jax.ShapeDtypeStruct
ANY = pl.BlockSpec(memory_space=pl.ANY)
C1 = 0.7978845608028654
C2 = C1 * 0.044715
CW = 768
VMEM_LIMIT = 63 * 2**20

SAME_CHIP = [(0, 1), (1, 0), (2, 3), (3, 2)]
CROSS_CHIP = [(0, 2), (1, 3), (2, 0), (3, 1)]


def dot_nn(a, b):
    return lax.dot_general(a, b, (((1,), (0,)), ((), ())), preferred_element_type=F32)


def dot_nt(a, b):
    return lax.dot_general(a, b, (((1,), (1,)), ((), ())), preferred_element_type=F32)


def gelu_gate(z):
    z2 = z * z
    return z2, 0.5 + 0.5 * jnp.tanh(z * (C1 + C2 * z2))


def gelu(z):
    return z * gelu_gate(z)[1]


def gelu_grad(z):
    z2, q = gelu_gate(z)
    return q + (z * (q * (1.0 - q))) * (2 * C1 + (6 * C2) * z2)


def load_weights(cands, bufs, sem):
    @pl.when(pl.program_id(0) == 0)
    def _():
        stage = lax.axis_index('stage')
        for k, cand in enumerate(cands):
            @pl.when(stage == k)
            def _(cand=cand):
                for i, (src, dst) in enumerate(zip(cand, bufs)):
                    pltpu.make_async_copy(src, dst, sem.at[i]).start()
        for i, (src, dst) in enumerate(zip(cands[0], bufs)):
            pltpu.make_async_copy(src, dst, sem.at[i]).wait()


def fwd_body(*refs, sub, save_a):
    h_ref, refs = refs[0], refs[2:]
    cands = [refs[4 * k:4 * k + 4] for k in range(4)]
    refs = refs[16:]
    za_ref, zb_ref, mid_ref, out_ref = refs[:4]
    refs = refs[4:]
    if save_a:
        aa_ref, ab_ref, refs = refs[0], refs[1], refs[2:]
    else:
        aa_ref, refs = refs[0], refs[1:]
    ua, wa, ub, wb, sem = refs
    load_weights(cands, (ua, wa, ub, wb), sem)
    rows, width = za_ref.shape
    for r in range(0, rows, sub):
        rs = slice(r, r + sub)
        h = h_ref[rs, :]
        for c in range(0, width, CW):
            cs = slice(c, c + CW)
            z = dot_nn(h, ua[:, cs])
            za_ref[rs, cs] = z
            aa_ref[rs, cs] = gelu(z).astype(BF)
        mid = (h.astype(F32) + dot_nn(aa_ref[rs, :], wa[...])).astype(BF)
        mid_ref[rs, :] = mid
        z = dot_nn(mid, ub[...])
        zb_ref[rs, :] = z
        a = gelu(z).astype(BF)
        if save_a:
            ab_ref[rs, :] = a
        out_ref[rs, :] = (mid.astype(F32) + dot_nn(a, wb[...])).astype(BF)


def weight_scratch(ws):
    return [pltpu.VMEM(w.shape, BF) for w in ws] + [pltpu.SemaphoreType.DMA((4,))]


def cost(flops, bytes_accessed):
    return pl.CostEstimate(flops=flops, bytes_accessed=bytes_accessed, transcendentals=0)


def fwd_pair(h, after, cands, save_a, rows=512, sub=256):
    n_tok, d = h.shape
    f, g = cands[0][0].shape[1], cands[0][2].shape[1]
    row = lambda n: pl.BlockSpec((rows, n), lambda i: (i, 0))
    outs = [(f, F32), (g, F32), (d, BF), (d, BF)] + ([(f, BF), (g, BF)] if save_a else [])
    scratch = ([] if save_a else [pltpu.VMEM((rows, f), BF)]) + weight_scratch(cands[0])
    return pl.pallas_call(
        functools.partial(fwd_body, sub=sub, save_a=save_a),
        grid=(n_tok // rows,),
        in_specs=[row(d)] + [ANY] * 17,
        out_specs=[row(n) for n, _ in outs],
        out_shape=[SDS((n_tok, n), t) for n, t in outs],
        scratch_shapes=scratch,
        cost_estimate=cost(4 * n_tok * d * (f + g), n_tok * (f + g) * 6),
        compiler_params=pltpu.CompilerParams(vmem_limit_bytes=VMEM_LIMIT),
        name='fwd_pair_a' if save_a else 'fwd_pair',
    )(h, after, *[w for cand in cands for w in cand])


def dgrad_body(*refs, sub, save_a):
    za_ref, zb_ref, g_ref, refs = refs[0], refs[1], refs[2], refs[4:]
    cands = [refs[4 * k:4 * k + 4] for k in range(4)]
    refs = refs[16:]
    dza_ref, dzb_ref, gm_ref, gp_ref = refs[:4]
    refs = refs[4:]
    if save_a:
        aa_ref, ab_ref, refs = refs[0], refs[1], refs[2:]
    ua, wa, ub, wb, sem = refs
    load_weights(cands, (ua, wa, ub, wb), sem)
    rows, width = za_ref.shape
    for r in range(0, rows, sub):
        rs = slice(r, r + sub)
        g = g_ref[rs, :]
        z = zb_ref[rs, :]
        if save_a:
            ab_ref[rs, :] = gelu(z).astype(BF)
        dz = (dot_nt(g, wb[...]) * gelu_grad(z)).astype(BF)
        dzb_ref[rs, :] = dz
        gm = (g.astype(F32) + dot_nt(dz, ub[...])).astype(BF)
        gm_ref[rs, :] = gm
        for c in range(0, width, CW):
            cs = slice(c, c + CW)
            z = za_ref[rs, cs]
            if save_a:
                aa_ref[rs, cs] = gelu(z).astype(BF)
            dza_ref[rs, cs] = (dot_nt(gm, wa[cs, :]) * gelu_grad(z)).astype(BF)
        gp_ref[rs, :] = (gm.astype(F32) + dot_nt(dza_ref[rs, :], ua[...])).astype(BF)


def dgrad_pair(za, zb, g, after, cands, save_a, rows=512, sub=256):
    n_tok, d = g.shape
    f, n = za.shape[1], zb.shape[1]
    row = lambda w: pl.BlockSpec((rows, w), lambda i: (i, 0))
    widths = [f, n, d, d] + ([f, n] if save_a else [])
    return pl.pallas_call(
        functools.partial(dgrad_body, sub=sub, save_a=save_a),
        grid=(n_tok // rows,),
        in_specs=[row(f), row(n), row(d)] + [ANY] * 17,
        out_specs=[row(w) for w in widths],
        out_shape=[SDS((n_tok, w), BF) for w in widths],
        scratch_shapes=weight_scratch(cands[0]),
        cost_estimate=cost(4 * n_tok * d * (f + n), n_tok * (f + n) * 6),
        compiler_params=pltpu.CompilerParams(vmem_limit_bytes=VMEM_LIMIT),
        name='dgrad_pair_a' if save_a else 'dgrad_pair',
    )(za, zb, g, after, *[w for cand in cands for w in cand])


def wgrad_body(*refs, ninit, phase, steps, rows, width):
    refs = refs[1:]
    cands = [refs[4 * k:4 * k + 4] for k in range(4)]
    refs = refs[16:]
    inits, out, refs = refs[:ninit], refs[ninit], refs[ninit + 1:]
    bufs, acc, refs = refs[:4], refs[4], refs[5:]
    if ninit:
        init_buf, refs = refs[0], refs[1:]
    sem, init_sem, out_sem = refs
    i = pl.program_id(0)
    stage = lax.axis_index('stage')
    kind = lax.rem(stage + phase, 2)
    sel = (stage // 2) * 2 + kind
    total = acc.shape[1]

    def tile_copies(step, slot, cand):
        rs = pl.ds(pl.multiple_of(step * rows, rows), rows)
        return [pltpu.make_async_copy(src.at[rs, :], dst.at[slot], sem.at[slot, k]) for k, (src, dst) in enumerate(zip(cand, bufs))]

    def start(step, slot):
        for k, cand in enumerate(cands):
            @pl.when(sel == k)
            def _(cand=cand):
                for cp in tile_copies(step, slot, cand):
                    cp.start()

    @pl.when(i == 0)
    def _():
        start(0, 0)
        for k in range(ninit):
            pltpu.make_async_copy(inits[k], init_buf.at[k], init_sem.at[k]).start()

    @pl.when(i + 1 < steps)
    def _():
        start(i + 1, (i + 1) % 2)

    slot = i % 2
    for cp in tile_copies(i, slot, cands[0]):
        cp.wait()
    xw, yw, xn, yn = [b.at[slot] for b in bufs]

    def product(mode):
        xt = xw[...].T
        for c in range(0, total, CW):
            cs = slice(c, c + CW)
            if c == width:
                xt = xn[...].T
            v = dot_nn(xt, yw[:, cs] if c < width else yn[:, c - width:c - width + CW])
            if mode == 'first':
                acc[:, cs] = v
            elif mode == 'mid':
                acc[:, cs] += v
            else:
                v = acc[:, cs] + v
                for k in range(ninit):
                    v = v + init_buf[k, :, cs]
                acc[:, cs] = v
                pltpu.make_async_copy(acc.at[:, cs], out.at[:, cs], out_sem.at[c // CW]).start()

    @pl.when(i == 0)
    def _():
        product('first')

    @pl.when((i > 0) & (i < steps - 1))
    def _():
        product('mid')

    @pl.when(i == steps - 1)
    def _():
        for k in range(ninit):
            pltpu.make_async_copy(inits[k], init_buf.at[k], init_sem.at[k]).wait()
        product('last')
        for c in range(0, total, CW):
            cs = slice(c, c + CW)
            pltpu.make_async_copy(acc.at[:, cs], out.at[:, cs], out_sem.at[c // CW]).wait()


def wgrad_half(after, pairs, phase, inits, rows=512):
    xw, yw, xn, yn = pairs[0][0]
    n_tok, d = xw.shape
    f, n = yw.shape[1], yn.shape[1]
    total = f + n
    scratch = [pltpu.VMEM((2, rows, w), BF) for w in (d, f, d, n)] + [pltpu.VMEM((d, total), F32)]
    if inits:
        scratch.append(pltpu.VMEM((len(inits), d, total), F32))
    scratch += [pltpu.SemaphoreType.DMA((2, 4)), pltpu.SemaphoreType.DMA((max(1, len(inits)),)), pltpu.SemaphoreType.DMA((total // CW,))]
    flat = [r for pair in pairs for cand in pair for r in cand]
    return pl.pallas_call(
        functools.partial(wgrad_body, ninit=len(inits), phase=phase, steps=n_tok // rows, rows=rows, width=f),
        grid=(n_tok // rows,),
        in_specs=[ANY] * (1 + len(flat) + len(inits)),
        out_specs=ANY,
        out_shape=SDS((d, total), F32),
        scratch_shapes=scratch,
        cost_estimate=cost(2 * n_tok * d * total, n_tok * total * 2),
        compiler_params=pltpu.CompilerParams(vmem_limit_bytes=VMEM_LIMIT),
        name=f'wgrad_{phase}_{len(inits)}',
    )(after, *flat, *inits)


def solution(mesh):
    tok_spec = P(('data', 'stage'))
    row_spec = P('stage')

    def device_body(acts_in, grad_out, w_up_a, w_down_a, w_up_b, w_down_b):
        n_micro, tokens, d = acts_in.shape
        n_tok = n_micro * tokens
        perm = lambda xs, pairs: tuple(lax.ppermute(x, 'stage', pairs) for x in xs)
        own = tuple(w[0] for w in (w_up_a, w_down_a, w_up_b, w_down_b))
        f = own[0].shape[1]

        peer = perm(own, SAME_CHIP)
        cross_even = perm(own, [(0, 2), (2, 0)])
        own_late, cross_even = lax.optimization_barrier((own, cross_even))
        far_odd = perm(cross_even, [(2, 3), (0, 1)])
        cross_odd = perm(own_late, [(1, 3), (3, 1)])
        far_even = perm(cross_odd, [(3, 2), (1, 0)])
        cands = [
            [own, peer, cross_even, far_odd],
            [peer, own, far_even, cross_odd],
            [cross_even, far_odd, own, peer],
            [far_even, cross_odd, peer, own],
        ]
        save_a = [True, True, False, False]

        h = acts_in.reshape(n_tok, d)
        saved = []
        after = h
        for j in range(4):
            outs = fwd_pair(h, after, cands[j], save_a[j])
            za, zb, mid, nxt = outs[:4]
            saved.append([h, mid, za, zb, *outs[4:]])
            h = after = nxt
        acts_out = h

        up_ops, down_ops = {}, {}
        g = grad_out.reshape(n_tok, d)

        def dgrad(j, g, after):
            h, mid, za, zb, *acts = saved[j]
            outs = dgrad_pair(za, zb, g, after, cands[j], not save_a[j])
            dza, dzb, gm, gp = outs[:4]
            aa, ab = acts if save_a[j] else outs[4:]
            up_ops[j] = (h, dza, mid, dzb)
            down_ops[j] = (gm, aa, g, ab)
            return gp

        def wgrad(after, pair0, pair1, phase, inits=()):
            pairs = [(up_ops[p], down_ops[p]) for p in (pair0, pair1)]
            return wgrad_half(after, pairs, phase, list(inits))

        swap = lambda x: lax.ppermute(x, 'stage', SAME_CHIP)
        cross = lambda x: lax.ppermute(x, 'stage', CROSS_CHIP)

        g = dgrad(3, g, after)
        g = dgrad(2, g, g)
        g = dgrad(1, g, g)
        a1 = wgrad(g, 3, 1, 0)
        a2 = wgrad(a1, 3, 1, 1, [swap(a1)])
        a_in = cross(a2)
        g = dgrad(0, g, a2)
        b1 = wgrad(g, 2, 0, 0)
        b2 = wgrad(b1, 2, 0, 1, [swap(b1)])
        b_in = cross(b2)
        c1 = wgrad(b2, 1, 3, 0)
        d1 = wgrad(c1, 0, 2, 0)
        c2 = wgrad(d1, 1, 3, 1, [swap(c1), a_in])
        d2 = wgrad(c2, 0, 2, 1, [swap(d1), b_in])
        c_in = lax.ppermute(c2, 'stage', [(0, 1), (2, 3)])
        d_in = lax.ppermute(d2, 'stage', [(1, 0), (3, 2)])
        odd = lax.axis_index('stage') % 2 == 1
        up = jnp.where(odd, c2, d_in)
        down = jnp.where(odd, c_in, d2)
        return (
            acts_out.reshape(acts_in.shape),
            g.reshape(acts_in.shape),
            up[None, :, :f],
            down[:, :f].T[None],
            up[None, :, f:],
            down[:, f:].T[None],
        )

    return jax.shard_map(device_body, mesh=mesh, in_specs=(tok_spec, tok_spec, row_spec, row_spec, row_spec, row_spec), out_specs=(tok_spec,) * 6, check_vma=False)
```

```python
import functools

import jax
import jax.numpy as jnp
from jax import lax
from jax.experimental import pallas as pl
from jax.experimental.pallas import tpu as pltpu
from jax.sharding import PartitionSpec as P


BF = jnp.bfloat16
F32 = jnp.float32
SDS = jax.ShapeDtypeStruct
ANY = pl.BlockSpec(memory_space=pl.ANY)
C1 = 0.7978845608028654
C2 = C1 * 0.044715
CW = 768
SAVE_A = [True, False, False, False]
VMEM_LIMIT = 63 * 2**20

SAME_CHIP = [(0, 1), (1, 0), (2, 3), (3, 2)]
CROSS_CHIP = [(0, 2), (1, 3), (2, 0), (3, 1)]


def dot_nn(a, b):
    return lax.dot_general(a, b, (((1,), (0,)), ((), ())), preferred_element_type=F32)


def dot_nt(a, b):
    return lax.dot_general(a, b, (((1,), (1,)), ((), ())), preferred_element_type=F32)


def gelu_gate(z):
    z2 = z * z
    return z2, 0.5 + 0.5 * jnp.tanh(z * (C1 + C2 * z2))


def gelu(z):
    return z * gelu_gate(z)[1]


def gelu_grad(z):
    z2, q = gelu_gate(z)
    return q + (z * (q * (1.0 - q))) * (2 * C1 + (6 * C2) * z2)


def load_weights(cands, bufs, sem):
    @pl.when(pl.program_id(0) == 0)
    def _():
        stage = lax.axis_index('stage')
        for k, cand in enumerate(cands):
            @pl.when(stage == k)
            def _(cand=cand):
                for i, (src, dst) in enumerate(zip(cand, bufs)):
                    pltpu.make_async_copy(src, dst, sem.at[i]).start()
        for i, (src, dst) in enumerate(zip(cands[0], bufs)):
            pltpu.make_async_copy(src, dst, sem.at[i]).wait()


def up_body(*refs):
    h_ref, cands, z_ref, u, sem = refs[0], refs[2:6], refs[6], refs[7], refs[8]
    load_weights([(c,) for c in cands], (u,), sem)
    h = h_ref[...]
    for c in range(0, z_ref.shape[1], CW):
        z_ref[:, c:c + CW] = dot_nn(h, u[:, c:c + CW])


def up_product(h, after, cands, rows=512):
    n_tok, d = h.shape
    f = cands[0].shape[1]
    row = lambda n: pl.BlockSpec((rows, n), lambda i: (i, 0))
    return pl.pallas_call(
        up_body,
        grid=(n_tok // rows,),
        in_specs=[row(d)] + [ANY] * 5,
        out_specs=row(f),
        out_shape=SDS((n_tok, f), F32),
        scratch_shapes=[pltpu.VMEM((d, f), BF), pltpu.SemaphoreType.DMA((1,))],
        cost_estimate=cost(2 * n_tok * d * f, n_tok * f * 4),
        compiler_params=pltpu.CompilerParams(vmem_limit_bytes=VMEM_LIMIT),
        name='up_product',
    )(h, after, *cands)


def fwd_body(*refs, sub, save_a, have_z):
    h_ref, refs = refs[0], refs[2:]
    first = 1 if have_z else 0
    cands = [refs[4 * k + first:4 * k + 4] for k in range(4)]
    refs = refs[16:]
    if have_z:
        za_in, zb_ref, mid_ref, out_ref = refs[:4]
    else:
        za_ref, zb_ref, mid_ref, out_ref = refs[:4]
    refs = refs[4:]
    if save_a:
        aa_ref, ab_ref, refs = refs[0], refs[1], refs[2:]
    else:
        aa_ref, refs = refs[0], refs[1:]
    if have_z:
        wa, ub, wb, sem = refs
        load_weights(cands, (wa, ub, wb), sem)
    else:
        ua, wa, ub, wb, sem = refs
        load_weights(cands, (ua, wa, ub, wb), sem)
    rows, width = aa_ref.shape
    for r in range(0, rows, sub):
        rs = slice(r, r + sub)
        h = h_ref[rs, :]
        for c in range(0, width, CW):
            cs = slice(c, c + CW)
            if have_z:
                z = za_in[rs, cs]
            else:
                z = dot_nn(h, ua[:, cs])
                za_ref[rs, cs] = z
            aa_ref[rs, cs] = gelu(z).astype(BF)
        mid = (h.astype(F32) + dot_nn(aa_ref[rs, :], wa[...])).astype(BF)
        mid_ref[rs, :] = mid
        z = dot_nn(mid, ub[...])
        zb_ref[rs, :] = z
        a = gelu(z).astype(BF)
        if save_a:
            ab_ref[rs, :] = a
        out_ref[rs, :] = (mid.astype(F32) + dot_nn(a, wb[...])).astype(BF)


def weight_scratch(ws):
    return [pltpu.VMEM(w.shape, BF) for w in ws] + [pltpu.SemaphoreType.DMA((len(ws),))]


def cost(flops, bytes_accessed):
    return pl.CostEstimate(flops=flops, bytes_accessed=bytes_accessed, transcendentals=0)


def fwd_pair(h, after, cands, save_a, za=None, rows=512, sub=256):
    n_tok, d = h.shape
    f, g = cands[0][0].shape[1], cands[0][2].shape[1]
    row = lambda n: pl.BlockSpec((rows, n), lambda i: (i, 0))
    have_z = za is not None
    outs = ([] if have_z else [(f, F32)]) + [(g, F32), (d, BF), (d, BF)] + ([(f, BF), (g, BF)] if save_a else [])
    scratch = ([] if save_a else [pltpu.VMEM((rows, f), BF)]) + weight_scratch(cands[0][1 if have_z else 0:])
    return pl.pallas_call(
        functools.partial(fwd_body, sub=sub, save_a=save_a, have_z=have_z),
        grid=(n_tok // rows,),
        in_specs=[row(d)] + [ANY] * 17 + ([row(f)] if have_z else []),
        out_specs=[row(n) for n, _ in outs],
        out_shape=[SDS((n_tok, n), t) for n, t in outs],
        scratch_shapes=scratch,
        cost_estimate=cost(4 * n_tok * d * (f + g) - (2 * n_tok * d * f if have_z else 0), n_tok * (f + g) * 6),
        compiler_params=pltpu.CompilerParams(vmem_limit_bytes=VMEM_LIMIT),
    )(h, after, *[w for cand in cands for w in cand], *([za] if have_z else []))


def dgrad_body(*refs, sub, save_a):
    za_ref, zb_ref, g_ref, refs = refs[0], refs[1], refs[2], refs[4:]
    cands = [refs[4 * k:4 * k + 4] for k in range(4)]
    refs = refs[16:]
    dza_ref, dzb_ref, gm_ref, gp_ref = refs[:4]
    refs = refs[4:]
    if save_a:
        aa_ref, ab_ref, refs = refs[0], refs[1], refs[2:]
    ua, wa, ub, wb, sem = refs
    load_weights(cands, (ua, wa, ub, wb), sem)
    rows, width = za_ref.shape
    for r in range(0, rows, sub):
        rs = slice(r, r + sub)
        g = g_ref[rs, :]
        z = zb_ref[rs, :]
        if save_a:
            ab_ref[rs, :] = gelu(z).astype(BF)
        dz = (dot_nt(g, wb[...]) * gelu_grad(z)).astype(BF)
        dzb_ref[rs, :] = dz
        gm = (g.astype(F32) + dot_nt(dz, ub[...])).astype(BF)
        gm_ref[rs, :] = gm
        for c in range(0, width, CW):
            cs = slice(c, c + CW)
            z = za_ref[rs, cs]
            if save_a:
                aa_ref[rs, cs] = gelu(z).astype(BF)
            dza_ref[rs, cs] = (dot_nt(gm, wa[cs, :]) * gelu_grad(z)).astype(BF)
        gp_ref[rs, :] = (gm.astype(F32) + dot_nt(dza_ref[rs, :], ua[...])).astype(BF)


def dgrad_pair(za, zb, g, after, cands, save_a, rows=512, sub=256):
    n_tok, d = g.shape
    f, n = za.shape[1], zb.shape[1]
    row = lambda w: pl.BlockSpec((rows, w), lambda i: (i, 0))
    widths = [f, n, d, d] + ([f, n] if save_a else [])
    return pl.pallas_call(
        functools.partial(dgrad_body, sub=sub, save_a=save_a),
        grid=(n_tok // rows,),
        in_specs=[row(f), row(n), row(d)] + [ANY] * 17,
        out_specs=[row(w) for w in widths],
        out_shape=[SDS((n_tok, w), BF) for w in widths],
        scratch_shapes=weight_scratch(cands[0]),
        cost_estimate=cost(4 * n_tok * d * (f + n), n_tok * (f + n) * 6),
        compiler_params=pltpu.CompilerParams(vmem_limit_bytes=VMEM_LIMIT),
        name='dgrad_pair_a' if save_a else 'dgrad_pair',
    )(za, zb, g, after, *[w for cand in cands for w in cand])


def wgrad_body(*refs, phase, steps, rows, wide, narrow, init_cols, col0):
    refs = refs[1:]
    cands = [refs[4 * k:4 * k + 4] for k in range(4)]
    refs = refs[16:]
    ninit = len(init_cols)
    inits, out, refs = refs[:ninit], refs[ninit], refs[ninit + 1:]
    nb = 4 if narrow else 2
    bufs, acc, refs = refs[:nb], refs[nb], refs[nb + 1:]
    init_bufs, refs = refs[:ninit], refs[ninit:]
    sem, init_sem, out_sem = refs
    i = pl.program_id(0)
    stage = lax.axis_index('stage')
    sel = (stage // 2) * 2 + lax.rem(stage + phase, 2)
    total = acc.shape[1]

    def tile_copies(step, slot, cand):
        rs = pl.ds(pl.multiple_of(step * rows, rows), rows)
        srcs = (cand[0].at[rs, :], cand[1].at[rs, pl.ds(col0, wide)], cand[2].at[rs, :], cand[3].at[rs, :])
        return [pltpu.make_async_copy(src, dst.at[slot], sem.at[slot, k]) for k, (src, dst) in enumerate(zip(srcs, bufs))]

    def init_copies():
        return [pltpu.make_async_copy(src, dst, init_sem.at[k]) for k, (src, dst) in enumerate(zip(inits, init_bufs))]

    def start(step, slot):
        for k, cand in enumerate(cands):
            @pl.when(sel == k)
            def _(cand=cand):
                for cp in tile_copies(step, slot, cand):
                    cp.start()

    @pl.when(i == 0)
    def _():
        start(0, 0)
        for cp in init_copies():
            cp.start()

    @pl.when(i + 1 < steps)
    def _():
        start(i + 1, (i + 1) % 2)

    slot = i % 2
    for cp in tile_copies(i, slot, cands[0]):
        cp.wait()
    tiles = [b.at[slot] for b in bufs]

    def product(mode):
        xt = tiles[0][...].T
        for c in range(0, total, CW):
            cs = slice(c, c + CW)
            if c == wide:
                xt = tiles[2][...].T
            v = dot_nn(xt, tiles[1][:, cs] if c < wide else tiles[3][:, c - wide:c - wide + CW])
            if mode == 'first':
                acc[:, cs] = v
            elif mode == 'mid':
                acc[:, cs] += v
            else:
                v = acc[:, cs] + v
                for (lo, hi), buf in zip(init_cols, init_bufs):
                    if lo <= c < hi:
                        v = v + buf[:, c - lo:c - lo + CW]
                acc[:, cs] = v
                pltpu.make_async_copy(acc.at[:, cs], out.at[:, cs], out_sem.at[c // CW]).start()

    @pl.when(i == 0)
    def _():
        product('first')

    @pl.when((i > 0) & (i < steps - 1))
    def _():
        product('mid')

    @pl.when(i == steps - 1)
    def _():
        for cp in init_copies():
            cp.wait()
        product('last')
        for c in range(0, total, CW):
            cs = slice(c, c + CW)
            pltpu.make_async_copy(acc.at[:, cs], out.at[:, cs], out_sem.at[c // CW]).wait()


def wgrad_half(after, pairs, phase, cols, inits):
    rows = 1024 if len(inits) < 2 else 512
    xw, yw, _, _ = pairs[0][0]
    n_tok, d = xw.shape
    f = yw.shape[1]
    lo, hi = cols
    wide, narrow = min(hi, f) - lo, max(hi - f, 0)
    total = wide + narrow
    widths = (d, wide, d, narrow) if narrow else (d, wide)
    scratch = [pltpu.VMEM((2, rows, w), BF) for w in widths] + [pltpu.VMEM((d, total), F32)]
    scratch += [pltpu.VMEM(arr.shape, F32) for arr, _ in inits]
    scratch += [pltpu.SemaphoreType.DMA((2, 4)), pltpu.SemaphoreType.DMA((max(1, len(inits)),)), pltpu.SemaphoreType.DMA((total // CW,))]
    flat = [r for pair in pairs for cand in pair for r in cand]
    return pl.pallas_call(
        functools.partial(wgrad_body, phase=phase, steps=n_tok // rows, rows=rows, wide=wide, narrow=narrow, init_cols=[c for _, c in inits], col0=lo),
        grid=(n_tok // rows,),
        in_specs=[ANY] * (1 + len(flat) + len(inits)),
        out_specs=ANY,
        out_shape=SDS((d, total), F32),
        scratch_shapes=scratch,
        cost_estimate=cost(2 * n_tok * d * total, n_tok * total * 2),
        compiler_params=pltpu.CompilerParams(vmem_limit_bytes=VMEM_LIMIT),
    )(after, *flat, *[arr for arr, _ in inits])


def final_body(_, odd_ref, even_ref, even_a, even_b, wide_ref, narrow_ref, *, flip):
    odd = lax.rem(lax.axis_index('stage'), 2) == 1
    f = wide_ref.shape[0 if flip else 1]

    def put(dst, v):
        if flip:
            dst[...] = v.T
        else:
            dst[...] = v

    @pl.when(odd)
    def _():
        put(wide_ref, odd_ref[:, :f])
        put(narrow_ref, odd_ref[:, f:])

    @pl.when(jnp.logical_not(odd))
    def _():
        extra = jnp.concatenate([even_a[...], even_b[...]], axis=1)
        v = even_ref[...] + extra
        put(wide_ref, v[:, :f])
        put(narrow_ref, v[:, f:])


def final_sum(after, odd_sum, even_sum, even_a, even_b, f, flip, rows=128):
    d, total = odd_sum.shape
    row = lambda n: pl.BlockSpec((rows, n), lambda i: (i, 0))
    col = lambda n: pl.BlockSpec((n, rows), lambda i: (0, i))
    n = total - f
    out = col if flip else row
    shape = (lambda w: (w, d)) if flip else (lambda w: (d, w))
    return pl.pallas_call(
        functools.partial(final_body, flip=flip),
        grid=(d // rows,),
        in_specs=[ANY, row(total), row(total), row(even_a.shape[1]), row(even_b.shape[1])],
        out_specs=[out(f), out(n)],
        out_shape=[SDS(shape(f), F32), SDS(shape(n), F32)],
        cost_estimate=cost(d * total * 512, d * total * 16),
        compiler_params=pltpu.CompilerParams(vmem_limit_bytes=VMEM_LIMIT),
        name='final_down' if flip else 'final_up',
    )(after, odd_sum, even_sum, even_a, even_b)


def solution(mesh):
    tok_spec = P(('data', 'stage'))
    row_spec = P('stage')

    def permute(x, pairs):
        return lax.ppermute(x, 'stage', pairs)

    def body(acts_in, grad_out, w_up_a, w_down_a, w_up_b, w_down_b):
        n_micro, tokens, d = acts_in.shape
        n_tok = n_micro * tokens
        permute_all = lambda xs, pairs: tuple(permute(x, pairs) for x in xs)
        own = tuple(w[0] for w in (w_up_a, w_down_a, w_up_b, w_down_b))
        f, n = own[0].shape[1], own[2].shape[1]
        half, total = f // 2, f + n

        cross_even = permute_all(own, [(0, 2), (2, 0)])
        peer = permute_all(own, SAME_CHIP)
        far_odd = permute_all(cross_even, [(2, 3), (0, 1)])
        own_late, _ = lax.optimization_barrier((own, cross_even))
        cross_odd = permute_all(own_late, [(1, 3), (3, 1)])
        far_even = permute_all(cross_odd, [(3, 2), (1, 0)])
        cands = [
            [own, peer, cross_even, far_odd],
            [peer, own, far_even, cross_odd],
            [cross_even, far_odd, own, peer],
            [far_even, cross_odd, peer, own],
        ]
        save_a = SAVE_A

        h = acts_in.reshape(n_tok, d)
        saved = []
        after = h
        for j in range(4):
            za = None
            if j < 2:
                za = after = up_product(h, after, [c[0] for c in cands[j]])
            outs = fwd_pair(h, after, cands[j], save_a[j], za)
            if za is not None:
                outs = [za, *outs]
            za, zb, mid, nxt = outs[:4]
            saved.append([h, mid, za, zb, *outs[4:]])
            h = after = nxt
        acts_out = h

        up_ops, down_ops = {}, {}
        g = grad_out.reshape(n_tok, d)

        def dgrad(j, g, after):
            h, mid, za, zb, *acts = saved[j]
            outs = dgrad_pair(za, zb, g, after, cands[j], not save_a[j])
            dza, dzb, gm, gp = outs[:4]
            aa, ab = acts if save_a[j] else outs[4:]
            up_ops[j] = (h, dza, mid, dzb)
            down_ops[j] = (gm, aa, g, ab)
            return gp

        def wgrad(after, pair0, pair1, phase, cols, inits=()):
            pairs = [(up_ops[p], down_ops[p]) for p in (pair0, pair1)]
            return wgrad_half(after, pairs, phase, cols, list(inits))

        swap = lambda x: permute(x, SAME_CHIP)
        part_a, part_b, whole = (0, half), (half, total), (0, total)

        g = dgrad(3, g, after)
        g = dgrad(2, g, g)
        g = dgrad(1, g, g)

        def two_phase(after, pair0, pair1):
            x1a = wgrad(after, pair0, pair1, 0, part_a)
            x1b = wgrad(x1a, pair0, pair1, 0, part_b)
            sa = swap(x1a)
            x2a = wgrad(x1b, pair0, pair1, 1, part_a, [(sa, (0, half))])
            sb = swap(x1b)
            x2b = wgrad(x2a, pair0, pair1, 1, part_b, [(sb, (0, total - half))])
            return x2a, x2b

        a2a, a2b = two_phase(g, 3, 1)
        in_a = permute(a2a, CROSS_CHIP)
        in_b = permute(a2b, CROSS_CHIP)
        g = dgrad(0, g, a2b)
        b2a, b2b = two_phase(g, 2, 0)
        bw_a = permute(b2a, [(0, 2), (2, 0)])
        bu_a = permute(b2a, [(1, 2), (3, 0)])
        bw_b = permute(b2b, [(0, 2), (2, 0)])
        bu_b = permute(b2b, [(1, 2), (3, 0)])
        c1 = wgrad(b2b, 1, 3, 0, whole)
        v1 = wgrad(c1, 0, 2, 0, whole)
        c2 = wgrad(v1, 1, 3, 1, whole, [(swap(c1), (0, total)), (in_a, (0, half)), (in_b, (half, total))])
        v2 = wgrad(c2, 0, 2, 1, whole, [(swap(v1), (0, total))])
        c_in = permute(c2, [(0, 1), (2, 3)])
        v_in = permute(v2, [(1, 0), (3, 2)])
        down_a, down_b = final_sum(v2, c_in, v2, bw_a, bw_b, f, True)
        up_a, up_b = final_sum(down_a, c2, v_in, bu_a, bu_b, f, False)
        return (
            acts_out.reshape(acts_in.shape),
            g.reshape(acts_in.shape),
            up_a[None],
            down_a[None],
            up_b[None],
            down_b[None],
        )

    return jax.shard_map(body, mesh=mesh, in_specs=(tok_spec, tok_spec, row_spec, row_spec, row_spec, row_spec), out_specs=(tok_spec,) * 6, check_vma=False)
```
